32 devices in a mesh: section: 8 (over z, y), tensor: 4 (over x, core).
Axes of the slice: x: 2, y: 2, z: 4, core: 2. Of those that a mesh axis runs over, the one named last changes fastest.
Arguments:
- section_input: bfloat16 [8, 512, 4096], P('section', 'tensor'), may hold values from -6 to 6
- history: bfloat16 [8, 1, 512, 4096], P('section', None, 'tensor'), may hold values from -6 to 6
- query_weight: bfloat16 [8, 4096, 3072], P('section', None, 'tensor'), may hold values from -0.4 to 0.4
- key_weight: bfloat16 [8, 4096, 512], P('section', None, 'tensor'), may hold values from -0.4 to 0.4
- value_weight: bfloat16 [8, 4096, 512], P('section', None, 'tensor'), may hold values from -0.09375 to 0.09375
- output_weight: bfloat16 [8, 3072, 4096], P('section', 'tensor'), may hold values from -0.5 to 0.5
- mix_weights: float32 [8, 2], replicated, may hold values from 0.2 to 0.6
Outputs:
- next_input: bfloat16 [8, 512, 4096], P('section', 'tensor')
The draws below stay inside these ranges and needn't reach their ends.
All inputs are finite; a program needn't handle non-finite values.
Results may differ from the reference program's by a relative error of at most 0.013.
The reference program's roundings to bfloat16 on the way count: a program that leaves them out, or rounds other values in their place, can miss the bound.
Values may be sent and summed in bfloat16 or wider, within the bound.
A program may use at most 128 MiB of HBM per device.

```python
import math
import jax
import jax.numpy as jnp
from jax import lax

D = 4096
HEADS = 48
KV_HEADS = 8
HEAD_DIM = 64
DILATION_STRIDE = 4
SEQ = 512
HIST = 1
N_SECTION = 8
N_TENSOR = 4


def draw_query_weight(key, part):
    entries = jax.random.normal(jax.random.fold_in(key, 11), (N_SECTION, D, HEADS * HEAD_DIM), jnp.float32) / jnp.sqrt(jnp.float32(D))
    return jnp.clip(entries, -0.39, 0.39).astype(jnp.bfloat16)


def draw_key_weight(key, part):
    entries = jax.random.normal(jax.random.fold_in(key, 13), (N_SECTION, D, KV_HEADS * HEAD_DIM), jnp.float32) / jnp.sqrt(jnp.float32(D))
    return jnp.clip(entries, -0.39, 0.39).astype(jnp.bfloat16)


def steps_of(rng, extent, shards, low, high):
    level, own = 1.0, jax.random.fold_in(rng, 6)
    for dim, shards_of in shards:
        heights = jnp.exp(jax.random.uniform(jax.random.fold_in(own, dim), (shards_of,), jnp.float32, low / len(shards), high / len(shards)))
        level = level * jnp.repeat(heights, extent[dim] // shards_of).reshape([-1 if axis == dim else 1 for axis in range(len(extent))])
    return level


def noise(key, shape, spread, reach, shards=(), kind=jnp.bfloat16):
    factor_of = steps_of(key, shape, shards, -0.22, 0.18) if shards else 1.0
    result = jax.random.normal(key, shape, jnp.float32) * spread * factor_of
    return jnp.minimum(jnp.maximum(result, -reach), reach).astype(kind)


def setup_inputs(seed: int = 0) -> dict:
    seeds = jax.random.split(jax.random.key(seed), 8)
    return {
        "section_input": noise(seeds[0], (N_SECTION, SEQ, D), 1.0, 6.0, ((0, 8), (1, 4))),
        "history": noise(seeds[1], (N_SECTION, HIST, SEQ, D), 1.0, 6.0, ((0, 8), (2, 4))),
        "query_weight": draw_query_weight(jax.random.fold_in(seeds[7], 71), 0),
        "key_weight": draw_key_weight(jax.random.fold_in(seeds[7], 71), 0),
        "value_weight": noise(seeds[4], (N_SECTION, D, KV_HEADS * HEAD_DIM), D ** -0.5, 0.09375, ((0, 8), (2, 4))),
        "output_weight": noise(seeds[5], (N_SECTION, HEADS * HEAD_DIM, D), 0.08, 0.5, ((0, 8), (1, 4))),
        "mix_weights": jnp.clip(jax.random.uniform(seeds[6], (N_SECTION, HIST + 1), jnp.float32, 0.2, 0.6), 0.2, 0.6),
    }


def normalize(token_rows):
    values = token_rows.astype(jnp.float32)
    inv_scale = lax.rsqrt(lax.optimization_barrier(jnp.mean(values * values, axis=-1, keepdims=True)) + 1e-05)
    return (values * inv_scale).astype(jnp.bfloat16)

def one_section(operands):
    token_rows, query_part, key_part, value_part, output_part = operands
    seq_len = token_rows.shape[0]
    normed = normalize(token_rows)
    query_rows = jnp.dot(normed, query_part, preferred_element_type=jnp.float32).astype(jnp.bfloat16)
    key_rows = jnp.dot(normed, key_part, preferred_element_type=jnp.float32).astype(jnp.bfloat16)
    value_rows = jnp.dot(normed, value_part, preferred_element_type=jnp.float32).astype(jnp.bfloat16)
    per_group = HEADS // KV_HEADS
    query_heads = query_rows.astype(jnp.float32).reshape(seq_len, KV_HEADS, per_group, HEAD_DIM)
    key_heads = key_rows.astype(jnp.float32).reshape(seq_len, KV_HEADS, HEAD_DIM)
    value_heads = value_rows.astype(jnp.float32).reshape(seq_len, KV_HEADS, HEAD_DIM)
    scores = jnp.einsum('tgjd,sgd->gjts', query_heads, key_heads) / math.sqrt(HEAD_DIM)
    positions = jnp.arange(seq_len, dtype=jnp.int32)
    scores = jnp.where(positions[:, None] >= positions[None, :], scores, -1e+30)
    softmax_weights = jax.nn.softmax(scores, axis=-1).astype(jnp.bfloat16)
    heads_out = jnp.einsum('gjts,sgd->tgjd', softmax_weights.astype(jnp.float32), value_heads)
    heads_out = heads_out.astype(jnp.bfloat16).reshape(seq_len, HEADS * HEAD_DIM)
    grouped = heads_out.astype(jnp.float32).reshape(seq_len, N_TENSOR, -1)
    grouped_weight = output_part.astype(jnp.float32).reshape(N_TENSOR, -1, D)
    partials = jnp.einsum('tnc,ncd->ntd', grouped, grouped_weight)
    partials = lax.optimization_barrier(partials.astype(jnp.bfloat16)).astype(jnp.float32)
    attention_sum = lax.optimization_barrier(jnp.sum(partials, axis=0))
    return (token_rows.astype(jnp.float32) + attention_sum).astype(jnp.bfloat16)

def reference(section_input, history, query_weight, key_weight, value_weight, output_weight, mix_weights):
    block_outs = lax.map(one_section, (section_input, query_weight, key_weight, value_weight, output_weight))
    section_numbers = jnp.arange(N_SECTION, dtype=jnp.int32)
    mixed_sum = mix_weights[:, 0][:, None, None] * block_outs.astype(jnp.float32)
    for history_slot in range(1, HIST + 1):
        sender_section = section_numbers - DILATION_STRIDE * history_slot
        picked = jnp.take(history[:, history_slot - 1], jnp.maximum(sender_section, 0).astype(jnp.int32), axis=0)
        factor = jnp.where(sender_section >= 0, mix_weights[:, history_slot], jnp.float32(0.0))
        mixed_sum = mixed_sum + factor[:, None, None] * picked.astype(jnp.float32)
    mixed = mixed_sum.astype(jnp.bfloat16)
    return jnp.concatenate([mixed[-1:], mixed[:-1]], axis=0)
```

```python
import functools
import math

import jax
import jax.numpy as jnp
from jax import lax
from jax.experimental import pallas as pl
from jax.experimental.pallas import tpu as pltpu
from jax.sharding import PartitionSpec as P

HEAD_DIM = 64
DILATION_STRIDE = 4
MESH = pl.DeviceIdType.MESH
LAG = 2


def start(copy):
    copy.start()
    return copy


def tick_kernel(
    sections,
    x_hbm,
    hist_hbm,
    wq_hbm,
    wk_hbm,
    wv_hbm,
    wo_hbm,
    mixw,
    out_hbm,
    x_own,
    chip_rows,
    peer_rows,
    w_all,
    w_out,
    q_all,
    k_pad,
    v_pad,
    heads,
    parts,
    sib_in,
    x_send,
    x_in,
    mixed,
    hist_in,
    w_sem,
    wo_sem,
    x_sem,
    hist_s,
    hist_r,
    sib_s,
    sib_r,
    gx_s,
    gx_r,
    fw_s,
    fw_r,
    rs_s,
    rs_r,
    xs_s,
    xs_r,
    out_s,
    out_r,
):
    section = lax.axis_index("section")
    me = lax.axis_index("tensor")
    hi, lo = me // 2, me % 2
    sibling = hi * 2 + (1 - lo)
    peer = (1 - hi) * 2 + lo
    rows, width = x_own.shape
    slots = hist_in.shape[0]
    chunks, both, _ = peer_rows.shape
    piece = both // 2
    q_tiles = w_all.shape[0] - 1
    tile = w_all.shape[2]
    half = tile // 2
    col_chunks, _, cols = w_out.shape
    nxt = lax.rem(section + 1, sections)
    prv = lax.rem(section + sections - 1, sections)

    load_x = start(pltpu.make_async_copy(x_hbm.at[0], x_own, x_sem))
    barrier = pltpu.get_barrier_semaphore()
    for other in (sibling, peer):
        pl.semaphore_signal(barrier, inc=1, device_id={"tensor": other}, device_id_type=MESH)
    for other in (nxt, prv):
        pl.semaphore_signal(barrier, inc=1, device_id={"section": other}, device_id_type=MESH)
    expected = jnp.int32(4)
    for k in range(1, slots + 1):
        step = DILATION_STRIDE * k
        forward, backward = section + step < sections, section >= step

        @pl.when(forward)
        def _():
            pl.semaphore_signal(
                barrier, inc=1, device_id={"section": section + step}, device_id_type=MESH
            )

        @pl.when(backward)
        def _():
            pl.semaphore_signal(
                barrier, inc=1, device_id={"section": section - step}, device_id_type=MESH
            )

        expected = expected + forward.astype(jnp.int32) + backward.astype(jnp.int32)

    loads = []
    for j in range(q_tiles):
        loads.append(
            pltpu.make_async_copy(
                wq_hbm.at[0, :, pl.ds(j * tile, tile)], w_all.at[j], w_sem.at[j]
            )
        )
    loads.append(
        pltpu.make_async_copy(
            wk_hbm.at[0], w_all.at[q_tiles, :, pl.ds(0, half)], w_sem.at[q_tiles]
        )
    )
    loads.append(
        pltpu.make_async_copy(
            wv_hbm.at[0], w_all.at[q_tiles, :, pl.ds(half, half)], w_sem.at[q_tiles + 1]
        )
    )
    load_x.wait()
    for copy in loads:
        copy.start()
    mine = pl.multiple_of(lo * rows, rows)

    def norm_rows(i, carry):
        at = pl.multiple_of(i * 16, 16)
        values = x_own[pl.ds(at, 16), :].astype(jnp.float32)
        inv = lax.rsqrt(jnp.mean(values * values, axis=-1, keepdims=True) + 1e-05)
        chip_rows[pl.ds(pl.multiple_of(mine + at, 16), 16), :] = (values * inv).astype(jnp.bfloat16)
        return carry

    lax.fori_loop(0, rows // 16, norm_rows, 0)
    pl.semaphore_wait(barrier, expected)

    def gather_copy(c):
        return pltpu.make_async_remote_copy(
            src_ref=chip_rows.at[pl.ds(pl.multiple_of(mine + c * piece, piece), piece)],
            dst_ref=peer_rows.at[c, pl.ds(pl.multiple_of(lo * piece, piece), piece)],
            send_sem=gx_s.at[c],
            recv_sem=gx_r.at[c],
            device_id={"tensor": peer},
            device_id_type=MESH,
        )

    def forward_copy(c):
        place = peer_rows.at[c, pl.ds(pl.multiple_of(lo * piece, piece), piece)]
        return pltpu.make_async_remote_copy(
            src_ref=place,
            dst_ref=place,
            send_sem=fw_s.at[c],
            recv_sem=fw_r.at[c],
            device_id={"tensor": sibling},
            device_id_type=MESH,
        )

    for c in range(chunks):
        gather_copy(c).start()
    own_place = chip_rows.at[pl.ds(mine, rows)]
    to_sibling = start(
        pltpu.make_async_remote_copy(
            src_ref=own_place,
            dst_ref=own_place,
            send_sem=sib_s,
            recv_sem=sib_r,
            device_id={"tensor": sibling},
            device_id_type=MESH,
        )
    )

    def hist_copy(k):
        return pltpu.make_async_remote_copy(
            src_ref=hist_hbm.at[0, k - 1],
            dst_ref=hist_in.at[k - 1],
            send_sem=hist_s.at[k - 1],
            recv_sem=hist_r.at[k - 1],
            device_id={"section": lax.rem(section + DILATION_STRIDE * k, sections)},
            device_id_type=MESH,
        )

    for k in range(1, slots + 1):
        step = DILATION_STRIDE * k

        @pl.when(section + step < sections)
        def _():
            hist_copy(k).start()

        @pl.when(section < step)
        def _():
            hist_in[k - 1] = jnp.zeros((rows, width), hist_in.dtype)

    out_loads = []
    for c in range(col_chunks):
        out_loads.append(
            start(
                pltpu.make_async_copy(
                    wo_hbm.at[0, :, pl.ds(c * cols, cols)], w_out.at[c], wo_sem.at[c]
                )
            )
        )

    scale = 1.0 / math.sqrt(HEAD_DIM)

    def project(rows_ref, spans):
        def q_tile(j, carry):
            acc = jnp.dot(rows_ref[...], w_all[j], preferred_element_type=jnp.float32)
            acc = (acc.astype(jnp.bfloat16) * jnp.bfloat16(scale)).astype(jnp.bfloat16)
            for source, target, size in spans:
                where = pl.ds(pl.multiple_of(target, size), size)
                q_all[2 * j, where, :] = acc[source : source + size, :half]
                q_all[2 * j + 1, where, :] = acc[source : source + size, half:]
            return carry

        lax.fori_loop(0, q_tiles, q_tile, 0)
        acc = jnp.dot(rows_ref[...], w_all[q_tiles], preferred_element_type=jnp.float32)
        acc = acc.astype(jnp.bfloat16).astype(jnp.float32)
        for part, padded in ((acc[:, :half], k_pad), (acc[:, half:], v_pad)):
            lane = lax.broadcasted_iota(jnp.int32, part.shape, 1)
            turned = pltpu.roll(part, HEAD_DIM, 1)
            low = lane < HEAD_DIM
            zero = jnp.zeros_like(part)
            forms = (
                jnp.where(low, part, zero),
                jnp.where(low, zero, turned),
                jnp.where(low, turned, zero),
                jnp.where(low, zero, part),
            )
            for f, form in enumerate(forms):
                form = form.astype(jnp.bfloat16)
                for source, target, size in spans:
                    where = pl.ds(pl.multiple_of(target, size), size)
                    padded[f, where, :] = form[source : source + size]

    for copy in loads:
        copy.wait()
    to_sibling.wait_recv()
    project(chip_rows, ((0, hi * 2 * rows, 2 * rows),))

    def peer_chunk(c, carry):
        gather_copy(c).wait_recv()
        forward_copy(c).start()
        forward_copy(c).wait_recv()
        base = (1 - hi) * 2 * rows + c * piece
        project(peer_rows.at[c], ((0, base, piece), (piece, base + rows, piece)))
        return carry

    lax.fori_loop(0, chunks, peer_chunk, 0)

    keys = k_pad.shape[1]
    pairs = q_all.shape[0]
    pairs_per_kv = pairs // (half // HEAD_DIM)

    def attend(side, first):
        def pair(p, carry):
            query = q_all[p, pl.ds(pl.multiple_of(first, 2 * rows), 2 * rows), :]
            row_at = first + lax.broadcasted_iota(jnp.int32, (2 * rows, keys), 0)
            key_at = lax.broadcasted_iota(jnp.int32, (2 * rows, keys), 1)
            seen = row_at >= key_at
            kv = p // pairs_per_kv
            total = None
            for which in range(2):
                scores = lax.dot_general(
                    query,
                    k_pad[kv * 2 + which],
                    (((1,), (1,)), ((), ())),
                    preferred_element_type=jnp.float32,
                )
                scores = jnp.where(seen, scores, -1e30)
                top = jnp.max(scores, axis=-1, keepdims=True)
                weights = jnp.exp(scores - top)
                weights = weights * (1.0 / jnp.sum(weights, axis=-1, keepdims=True))
                term = jnp.dot(
                    weights.astype(jnp.bfloat16),
                    v_pad[kv * 2 + which],
                    preferred_element_type=jnp.float32,
                )
                total = term if total is None else total + term
            heads[side, :, pl.ds(pl.multiple_of(p * half, half), half)] = total.astype(jnp.bfloat16)
            return carry

        lax.fori_loop(0, pairs, pair, 0)

    def sib_copy(side, c):
        return pltpu.make_async_remote_copy(
            src_ref=parts.at[side, c, 1 - lo],
            dst_ref=sib_in.at[side, c],
            send_sem=rs_s.at[side, c],
            recv_sem=rs_r.at[side, c],
            device_id={"tensor": sibling},
            device_id_type=MESH,
        )

    def peer_copy(c):
        return pltpu.make_async_remote_copy(
            src_ref=x_send.at[c],
            dst_ref=x_in.at[c],
            send_sem=xs_s.at[c],
            recv_sem=xs_r.at[c],
            device_id={"tensor": peer},
            device_id_type=MESH,
        )

    def out_copy(c):
        return pltpu.make_async_remote_copy(
            src_ref=mixed.at[c],
            dst_ref=out_hbm.at[0, :, pl.ds(pl.multiple_of(c * cols, cols), cols)],
            send_sem=out_s.at[c],
            recv_sem=out_r.at[c],
            device_id={"section": nxt},
            device_id_type=MESH,
        )

    def make_part(side, c):
        acc = jnp.dot(heads[side], w_out[c], preferred_element_type=jnp.float32)
        acc = acc.astype(jnp.bfloat16)
        parts[side, c, 0] = acc[:rows]
        parts[side, c, 1] = acc[rows:]
        sib_copy(side, c).start()

    def pair_sum(side, c):
        sib_copy(side, c).wait_recv()
        return parts[side, c, lo].astype(jnp.float32) + sib_in[side, c].astype(jnp.float32)

    attend(0, (1 - hi) * 2 * rows)
    for copy in out_loads:
        copy.wait()

    def peer_step(c, carry):
        @pl.when(c < col_chunks)
        def _():
            make_part(0, c)

        @pl.when(c >= LAG)
        def _():
            x_send[c - LAG] = pair_sum(0, c - LAG).astype(jnp.bfloat16)
            peer_copy(c - LAG).start()

        return carry

    lax.fori_loop(0, col_chunks + LAG, peer_step, 0)
    attend(1, hi * 2 * rows)

    def own_step(c, carry):
        make_part(1, c)
        return carry

    lax.fori_loop(0, col_chunks, own_step, 0)
    for k in range(1, slots + 1):

        @pl.when(section >= DILATION_STRIDE * k)
        def _():
            hist_copy(k).wait_recv()

    def final_step(c, carry):
        total = pair_sum(1, c)
        where = pl.ds(pl.multiple_of(c * cols, cols), cols)
        peer_copy(c).wait_recv()
        total = total + x_in[c].astype(jnp.float32)
        block = (x_own[:, where].astype(jnp.float32) + total).astype(jnp.bfloat16)
        value = mixw[section, 0] * block.astype(jnp.float32)
        for k in range(1, slots + 1):
            value = value + mixw[section, k] * hist_in[k - 1, :, where].astype(jnp.float32)
        mixed[c] = value.astype(jnp.bfloat16)
        out_copy(c).start()
        return carry

    lax.fori_loop(0, col_chunks, final_step, 0)

    to_sibling.wait_send()

    def drain_gather(c, carry):
        gather_copy(c).wait_send()
        forward_copy(c).wait_send()
        return carry

    lax.fori_loop(0, chunks, drain_gather, 0)
    for k in range(1, slots + 1):

        @pl.when(section + DILATION_STRIDE * k < sections)
        def _():
            hist_copy(k).wait_send()

    def drain(c, carry):
        sib_copy(0, c).wait_send()
        sib_copy(1, c).wait_send()
        peer_copy(c).wait_send()
        out_copy(c).wait()
        return carry

    lax.fori_loop(0, col_chunks, drain, 0)


def solution(mesh):
    sections, tensor = mesh.shape["section"], mesh.shape["tensor"]
    chunks, col_chunks = 2, 8

    def on_device(x, history, wq, wk, wv, wo, mix_weights):
        rows, width = x.shape[1:]
        slots = history.shape[1]
        q_width, kv_width = wq.shape[2], wk.shape[2]
        seq = rows * tensor
        tile = 2 * kv_width
        q_tiles = q_width // tile
        cols = width // col_chunks
        bf16 = jnp.bfloat16
        dma = pltpu.SemaphoreType.DMA
        hbm = pl.BlockSpec(memory_space=pl.ANY)
        piece = rows // chunks
        return pl.pallas_call(
            functools.partial(tick_kernel, sections),
            out_shape=jax.ShapeDtypeStruct(x.shape, bf16),
            in_specs=[hbm] * 6 + [pl.BlockSpec(memory_space=pltpu.SMEM)],
            out_specs=hbm,
            scratch_shapes=[
                pltpu.VMEM((rows, width), bf16),
                pltpu.VMEM((2 * rows, width), bf16),
                pltpu.VMEM((chunks, 2 * piece, width), bf16),
                pltpu.VMEM((q_tiles + 1, width, tile), bf16),
                pltpu.VMEM((col_chunks, q_width, cols), bf16),
                pltpu.VMEM((2 * q_tiles, seq, kv_width), bf16),
                pltpu.VMEM((4, seq, kv_width), bf16),
                pltpu.VMEM((4, seq, kv_width), bf16),
                pltpu.VMEM((2, 2 * rows, q_width), bf16),
                pltpu.VMEM((2, col_chunks, 2, rows, cols), bf16),
                pltpu.VMEM((2, col_chunks, rows, cols), bf16),
                pltpu.VMEM((col_chunks, rows, cols), bf16),
                pltpu.VMEM((col_chunks, rows, cols), bf16),
                pltpu.VMEM((col_chunks, rows, cols), bf16),
                pltpu.VMEM((slots, rows, width), bf16),
                dma((q_tiles + 2,)),
                dma((col_chunks,)),
                dma,
                dma((slots,)),
                dma((slots,)),
                dma,
                dma,
                dma((chunks,)),
                dma((chunks,)),
                dma((chunks,)),
                dma((chunks,)),
                dma((2, col_chunks)),
                dma((2, col_chunks)),
                dma((col_chunks,)),
                dma((col_chunks,)),
                dma((col_chunks,)),
                dma((col_chunks,)),
            ],
            compiler_params=pltpu.CompilerParams(
                collective_id=0, has_side_effects=True, vmem_limit_bytes=60 * 1024 * 1024
            ),
        )(x, history, wq, wk, wv, wo, mix_weights)

    placed = (
        P("section", "tensor", None),
        P("section", None, "tensor", None),
        P("section", None, "tensor"),
        P("section", None, "tensor"),
        P("section", None, "tensor"),
        P("section", "tensor", None),
        P(),
    )
    return jax.shard_map(
        on_device,
        mesh=mesh,
        in_specs=placed,
        out_specs=P("section", "tensor", None),
        check_vma=False,
    )
```

```python
import functools
import math

import jax
import jax.numpy as jnp
from jax import lax
from jax.experimental import pallas as pl
from jax.experimental.pallas import tpu as pltpu
from jax.sharding import PartitionSpec as P

HEAD_DIM = 64
DILATION_STRIDE = 4
MESH = pl.DeviceIdType.MESH
LAG = 2


def start(copy):
    copy.start()
    return copy


def tick_kernel(
    sections,
    x_hbm,
    hist_hbm,
    wq_hbm,
    wk_hbm,
    wv_hbm,
    wo_hbm,
    mix_hbm,
    out_hbm,
    x_own,
    chip_rows,
    peer_rows,
    w_all,
    w_out,
    q_all,
    k_pad,
    v_pad,
    peer_heads,
    own_heads,
    peer_keep,
    peer_give,
    peer_got,
    own_parts,
    own_got,
    x_in,
    mixed,
    hist_in,
    mix_v,
    w_sem,
    wo_sem,
    x_sem,
    mix_sem,
    hist_s,
    hist_r,
    sib_s,
    sib_r,
    gx_s,
    gx_r,
    fw_s,
    fw_r,
    ps_s,
    ps_r,
    os_s,
    os_r,
    xs_s,
    xs_r,
    out_s,
    out_r,
):
    section = lax.axis_index("section")
    me = lax.axis_index("tensor")
    hi, lo = me // 2, me % 2
    sibling = hi * 2 + (1 - lo)
    peer = (1 - hi) * 2 + lo
    rows, width = x_own.shape
    slots = hist_in.shape[0]
    piece = rows // 2
    q_tiles = w_all.shape[0] - 1
    tile = w_all.shape[2]
    half = tile // 2
    col_chunks, _, cols = w_out.shape
    side = col_chunks // 2
    nxt = lax.rem(section + 1, sections)
    prv = lax.rem(section + sections - 1, sections)

    load_x = start(pltpu.make_async_copy(x_hbm.at[0], x_own, x_sem))
    barrier = pltpu.get_barrier_semaphore()
    for other in (sibling, peer, (1 - hi) * 2 + (1 - lo)):
        pl.semaphore_signal(barrier, inc=1, device_id={"tensor": other}, device_id_type=MESH)
    for other in (nxt, prv):
        pl.semaphore_signal(barrier, inc=1, device_id={"section": other}, device_id_type=MESH)
    expected = jnp.int32(5)
    for k in range(1, slots + 1):
        step = DILATION_STRIDE * k
        forward, backward = section + step < sections, section >= step

        @pl.when(forward)
        def _():
            pl.semaphore_signal(
                barrier, inc=1, device_id={"section": section + step}, device_id_type=MESH
            )

        @pl.when(backward)
        def _():
            pl.semaphore_signal(
                barrier, inc=1, device_id={"section": section - step}, device_id_type=MESH
            )

        expected = expected + forward.astype(jnp.int32) + backward.astype(jnp.int32)

    loads = []
    for j in range(q_tiles):
        loads.append(
            pltpu.make_async_copy(
                wq_hbm.at[0, :, pl.ds(j * tile, tile)], w_all.at[j], w_sem.at[j]
            )
        )
    loads.append(
        pltpu.make_async_copy(
            wk_hbm.at[0], w_all.at[q_tiles, :, pl.ds(0, half)], w_sem.at[q_tiles]
        )
    )
    loads.append(
        pltpu.make_async_copy(
            wv_hbm.at[0], w_all.at[q_tiles, :, pl.ds(half, half)], w_sem.at[q_tiles + 1]
        )
    )
    load_x.wait()
    for copy in loads:
        copy.start()
    load_mix = start(pltpu.make_async_copy(mix_hbm, mix_v, mix_sem))
    mine = pl.multiple_of(lo * rows, rows)

    def norm_rows(i, carry):
        at = pl.multiple_of(i * 16, 16)
        values = x_own[pl.ds(at, 16), :].astype(jnp.float32)
        inv = lax.rsqrt(jnp.mean(values * values, axis=-1, keepdims=True) + 1e-05)
        chip_rows[pl.ds(pl.multiple_of(mine + at, 16), 16), :] = (values * inv).astype(jnp.bfloat16)
        return carry

    lax.fori_loop(0, rows // 16, norm_rows, 0)
    pl.semaphore_wait(barrier, expected)

    def gather_copy(j):
        return pltpu.make_async_remote_copy(
            src_ref=chip_rows.at[pl.ds(pl.multiple_of(j * rows + lo * piece, piece), piece)],
            dst_ref=peer_rows.at[j, pl.ds(pl.multiple_of(lo * piece, piece), piece)],
            send_sem=gx_s.at[j],
            recv_sem=gx_r.at[j],
            device_id={"tensor": peer},
            device_id_type=MESH,
        )

    def forward_copy(j):
        place = peer_rows.at[j, pl.ds(pl.multiple_of(lo * piece, piece), piece)]
        return pltpu.make_async_remote_copy(
            src_ref=place,
            dst_ref=place,
            send_sem=fw_s.at[j],
            recv_sem=fw_r.at[j],
            device_id={"tensor": sibling},
            device_id_type=MESH,
        )

    def sibling_copy(i):
        which = 1 - lo if i == 0 else lo
        place = chip_rows.at[pl.ds(pl.multiple_of(mine + which * piece, piece), piece)]
        return pltpu.make_async_remote_copy(
            src_ref=place,
            dst_ref=place,
            send_sem=sib_s.at[i],
            recv_sem=sib_r.at[i],
            device_id={"tensor": sibling},
            device_id_type=MESH,
        )

    @pl.when(lo == 0)
    def _():
        gather_copy(0).start()

    for i in range(2):
        sibling_copy(i).start()
    sibling_copy(0).wait_recv()

    @pl.when(lo == 1)
    def _():
        gather_copy(0).start()

    gather_copy(1).start()

    def hist_copy(k):
        return pltpu.make_async_remote_copy(
            src_ref=hist_hbm.at[0, k - 1],
            dst_ref=hist_in.at[k - 1],
            send_sem=hist_s.at[k - 1],
            recv_sem=hist_r.at[k - 1],
            device_id={"section": lax.rem(section + DILATION_STRIDE * k, sections)},
            device_id_type=MESH,
        )

    for k in range(1, slots + 1):
        step = DILATION_STRIDE * k

        @pl.when(section + step < sections)
        def _():
            hist_copy(k).start()

        @pl.when(section < step)
        def _():
            hist_in[k - 1] = jnp.zeros((rows, width), hist_in.dtype)

    out_loads = []
    for c in range(col_chunks):
        out_loads.append(
            start(
                pltpu.make_async_copy(
                    wo_hbm.at[0, :, pl.ds(c * cols, cols)], w_out.at[c], wo_sem.at[c]
                )
            )
        )

    scale = 1.0 / math.sqrt(HEAD_DIM)

    def project(rows_ref, target):
        size = rows_ref.shape[0]
        where = pl.ds(pl.multiple_of(target, size), size)

        def q_tile(j, carry):
            acc = jnp.dot(rows_ref[...], w_all[j], preferred_element_type=jnp.float32)
            acc = acc.astype(jnp.bfloat16) * jnp.bfloat16(scale)
            q_all[2 * j, where, :] = acc[:, :half]
            q_all[2 * j + 1, where, :] = acc[:, half:]
            return carry

        lax.fori_loop(0, q_tiles, q_tile, 0)
        acc = jnp.dot(rows_ref[...], w_all[q_tiles], preferred_element_type=jnp.float32)
        acc = acc.astype(jnp.bfloat16).astype(jnp.float32)
        for part, padded in ((acc[:, :half], k_pad), (acc[:, half:], v_pad)):
            lane = lax.broadcasted_iota(jnp.int32, part.shape, 1)
            turned = pltpu.roll(part, HEAD_DIM, 1)
            low = lane < HEAD_DIM
            zero = jnp.zeros_like(part)
            forms = (
                jnp.where(low, part, zero),
                jnp.where(low, zero, turned),
                jnp.where(low, turned, zero),
                jnp.where(low, zero, part),
            )
            for f, form in enumerate(forms):
                padded[f, where, :] = form.astype(jnp.bfloat16)

    pairs = q_all.shape[0]
    pairs_per_kv = pairs // (half // HEAD_DIM)

    def attend(heads_ref, first, size, keys):
        def pair(p, carry):
            query = q_all[p, first : first + size, :]
            row_at = first + lax.broadcasted_iota(jnp.int32, (size, keys), 0)
            key_at = lax.broadcasted_iota(jnp.int32, (size, keys), 1)
            seen = row_at >= key_at
            kv = p // pairs_per_kv
            total = None
            for which in range(2):
                scores = lax.dot_general(
                    query,
                    k_pad[kv * 2 + which, :keys, :],
                    (((1,), (1,)), ((), ())),
                    preferred_element_type=jnp.float32,
                )
                scores = jnp.where(seen, scores, -1e30)
                top = jnp.max(scores, axis=-1, keepdims=True)
                weights = jnp.exp(scores - top)
                weights = weights * (1.0 / jnp.sum(weights, axis=-1, keepdims=True))
                term = jnp.dot(
                    weights.astype(jnp.bfloat16),
                    v_pad[kv * 2 + which, :keys, :],
                    preferred_element_type=jnp.float32,
                )
                total = term if total is None else total + term
            heads_ref[:, pl.ds(pl.multiple_of(p * half, half), half)] = total.astype(jnp.bfloat16)
            return carry

        lax.fori_loop(0, pairs, pair, 0)

    def give_copy(j, i):
        return pltpu.make_async_remote_copy(
            src_ref=peer_give.at[j, i],
            dst_ref=peer_got.at[j, i],
            send_sem=ps_s.at[j, i],
            recv_sem=ps_r.at[j, i],
            device_id={"tensor": sibling},
            device_id_type=MESH,
        )

    def cross_copy(j, i):
        return pltpu.make_async_remote_copy(
            src_ref=peer_keep.at[j, i],
            dst_ref=x_in.at[lo * side + i],
            send_sem=xs_s.at[j, i],
            recv_sem=xs_r.at[lo * side + i],
            device_id={"tensor": (1 - hi) * 2 + j},
            device_id_type=MESH,
        )

    def cross_arrival(c):
        return pltpu.make_async_remote_copy(
            src_ref=x_in.at[c],
            dst_ref=x_in.at[c],
            send_sem=xs_s.at[0, 0],
            recv_sem=xs_r.at[c],
            device_id={"tensor": peer},
            device_id_type=MESH,
        )

    def peer_output(j):
        def part(c):
            acc = jnp.dot(peer_heads[j], w_out[c], preferred_element_type=jnp.float32)
            return acc.astype(jnp.bfloat16)

        def step(i, carry):
            @pl.when(i < side)
            def _():
                peer_give[j, i] = part((1 - lo) * side + i)
                peer_keep[j, i] = part(lo * side + i)
                give_copy(j, i).start()

            @pl.when(i >= LAG)
            def _():
                at = i - LAG
                give_copy(j, at).wait_recv()
                total = peer_keep[j, at].astype(jnp.float32) + peer_got[j, at].astype(jnp.float32)
                peer_keep[j, at] = total.astype(jnp.bfloat16)
                cross_copy(j, at).start()

            return carry

        lax.fori_loop(0, side + LAG, step, 0)

    def own_copy(c):
        return pltpu.make_async_remote_copy(
            src_ref=own_parts.at[c, 1 - lo],
            dst_ref=own_got.at[c],
            send_sem=os_s.at[c],
            recv_sem=os_r.at[c],
            device_id={"tensor": sibling},
            device_id_type=MESH,
        )

    def own_part(c):
        acc = jnp.dot(own_heads[...], w_out[c], preferred_element_type=jnp.float32)
        acc = acc.astype(jnp.bfloat16)
        own_parts[c, 0] = acc[:rows]
        own_parts[c, 1] = acc[rows:]
        own_copy(c).start()

    def out_copy(c):
        return pltpu.make_async_remote_copy(
            src_ref=mixed.at[c],
            dst_ref=out_hbm.at[0, :, pl.ds(pl.multiple_of(c * cols, cols), cols)],
            send_sem=out_s.at[c],
            recv_sem=out_r.at[c],
            device_id={"section": nxt},
            device_id_type=MESH,
        )

    for copy in loads:
        copy.wait()
    sibling_copy(1).wait_recv()
    project(chip_rows, hi * 2 * rows)
    for copy in out_loads:
        copy.wait()
    load_mix.wait()

    @pl.when(hi == 0)
    def _():
        attend(own_heads, 0, 2 * rows, 2 * rows)

        def own_step(c, carry):
            own_part(c)
            return carry

        lax.fori_loop(0, col_chunks, own_step, 0)

    for j in range(2):
        gather_copy(j).wait_recv()
        forward_copy(j).start()
        forward_copy(j).wait_recv()
        project(peer_rows.at[j], ((1 - hi) * 2 + j) * rows)

        @pl.when(hi == 0)
        def _():
            attend(peer_heads.at[j], (2 + j) * rows, rows, (3 + j) * rows)

        @pl.when(hi == 1)
        def _():
            attend(peer_heads.at[j], j * rows, rows, (1 + j) * rows)

        peer_output(j)

    @pl.when(hi == 1)
    def _():
        attend(own_heads, 2 * rows, 2 * rows, 4 * rows)

    for k in range(1, slots + 1):

        @pl.when(section >= DILATION_STRIDE * k)
        def _():
            hist_copy(k).wait_recv()

    def final_chunk(c):
        own_copy(c).wait_recv()
        total = own_parts[c, lo].astype(jnp.float32) + own_got[c].astype(jnp.float32)
        where = pl.ds(pl.multiple_of(c * cols, cols), cols)
        cross_arrival(c).wait_recv()
        total = total + x_in[c].astype(jnp.float32)
        block = (x_own[:, where].astype(jnp.float32) + total).astype(jnp.bfloat16)
        factors = mix_v[pl.ds(section, 1), :]
        value = factors[:, 0:1] * block.astype(jnp.float32)
        for k in range(1, slots + 1):
            past = hist_in[k - 1, :, where].astype(jnp.float32)
            value = value + factors[:, k : k + 1] * past
        mixed[c] = value.astype(jnp.bfloat16)
        out_copy(c).start()

    def column(i):
        return (i % 2) * side + i // 2

    def final_step(i, carry):
        @pl.when((i < col_chunks) & (hi == 1))
        def _():
            own_part(column(i))

        @pl.when(i >= LAG)
        def _():
            final_chunk(column(i - LAG))

        return carry

    lax.fori_loop(0, col_chunks + LAG, final_step, 0)

    for i in range(2):
        sibling_copy(i).wait_send()
        gather_copy(i).wait_send()
        forward_copy(i).wait_send()
    for k in range(1, slots + 1):

        @pl.when(section + DILATION_STRIDE * k < sections)
        def _():
            hist_copy(k).wait_send()

    def drain(c, carry):
        j, i = c // side, c % side
        give_copy(j, i).wait_send()
        cross_copy(j, i).wait_send()
        own_copy(c).wait_send()
        out_copy(c).wait()
        return carry

    lax.fori_loop(0, col_chunks, drain, 0)


def solution(mesh):
    sections, tensor = mesh.shape["section"], mesh.shape["tensor"]
    assert tensor == 4
    col_chunks = 8

    def on_device(x, history, wq, wk, wv, wo, mix_weights):
        rows, width = x.shape[1:]
        slots = history.shape[1]
        q_width, kv_width = wq.shape[2], wk.shape[2]
        seq = rows * tensor
        tile = 2 * kv_width
        q_tiles = q_width // tile
        cols = width // col_chunks
        bf16 = jnp.bfloat16
        dma = pltpu.SemaphoreType.DMA
        hbm = pl.BlockSpec(memory_space=pl.ANY)
        return pl.pallas_call(
            functools.partial(tick_kernel, sections),
            out_shape=jax.ShapeDtypeStruct(x.shape, bf16),
            in_specs=[hbm] * 7,
            out_specs=hbm,
            scratch_shapes=[
                pltpu.VMEM((rows, width), bf16),
                pltpu.VMEM((2 * rows, width), bf16),
                pltpu.VMEM((2, rows, width), bf16),
                pltpu.VMEM((q_tiles + 1, width, tile), bf16),
                pltpu.VMEM((col_chunks, q_width, cols), bf16),
                pltpu.VMEM((2 * q_tiles, seq, kv_width), bf16),
                pltpu.VMEM((4, seq, kv_width), bf16),
                pltpu.VMEM((4, seq, kv_width), bf16),
                pltpu.VMEM((2, rows, q_width), bf16),
                pltpu.VMEM((2 * rows, q_width), bf16),
                pltpu.VMEM((2, col_chunks // 2, rows, cols), bf16),
                pltpu.VMEM((2, col_chunks // 2, rows, cols), bf16),
                pltpu.VMEM((2, col_chunks // 2, rows, cols), bf16),
                pltpu.VMEM((col_chunks, 2, rows, cols), bf16),
                pltpu.VMEM((col_chunks, rows, cols), bf16),
                pltpu.VMEM((col_chunks, rows, cols), bf16),
                pltpu.VMEM((col_chunks, rows, cols), bf16),
                pltpu.VMEM((slots, rows, width), bf16),
                pltpu.VMEM(mix_weights.shape, mix_weights.dtype),
                dma((q_tiles + 2,)),
                dma((col_chunks,)),
                dma,
                dma,
                dma((slots,)),
                dma((slots,)),
                dma((2,)),
                dma((2,)),
                dma((2,)),
                dma((2,)),
                dma((2,)),
                dma((2,)),
                dma((2, col_chunks // 2)),
                dma((2, col_chunks // 2)),
                dma((col_chunks,)),
                dma((col_chunks,)),
                dma((2, col_chunks // 2)),
                dma((col_chunks,)),
                dma((col_chunks,)),
                dma((col_chunks,)),
            ],
            compiler_params=pltpu.CompilerParams(
                collective_id=0, has_side_effects=True, vmem_limit_bytes=60 * 1024 * 1024
            ),
        )(x, history, wq, wk, wv, wo, mix_weights)

    placed = (
        P("section", "tensor", None),
        P("section", None, "tensor", None),
        P("section", None, "tensor"),
        P("section", None, "tensor"),
        P("section", None, "tensor"),
        P("section", "tensor", None),
        P(),
    )
    return jax.shard_map(
        on_device,
        mesh=mesh,
        in_specs=placed,
        out_specs=P("section", "tensor", None),
        check_vma=False,
    )
```

```python
import functools
import math

import jax
import jax.numpy as jnp
from jax import lax
from jax.experimental import pallas as pl
from jax.experimental.pallas import tpu as pltpu
from jax.sharding import PartitionSpec as P

HEAD_DIM = 64
DILATION_STRIDE = 4
MESH = pl.DeviceIdType.MESH
LAG = 2


def start(copy):
    copy.start()
    return copy


def tick_kernel(
    sections,
    x_hbm,
    hist_hbm,
    wq_hbm,
    wk_hbm,
    wv_hbm,
    wo_hbm,
    mix_hbm,
    out_hbm,
    x_own,
    chip_rows,
    peer_rows,
    w_all,
    w_out,
    q_all,
    k_pad,
    v_pad,
    peer_heads,
    own_heads,
    peer_keep,
    peer_give,
    peer_got,
    own_parts,
    own_got,
    x_in,
    mixed,
    hist_in,
    mix_v,
    w_sem,
    wo_sem,
    x_sem,
    mix_sem,
    hist_s,
    hist_r,
    sib_s,
    sib_r,
    gx_s,
    gx_r,
    fw_s,
    fw_r,
    ps_s,
    ps_r,
    os_s,
    os_r,
    xs_s,
    xs_r,
    out_s,
    out_r,
    block_in,
    store_sem,
):
    section = lax.axis_index("section")
    me = lax.axis_index("tensor")
    hi, lo = me // 2, me % 2
    sibling = hi * 2 + (1 - lo)
    peer = (1 - hi) * 2 + lo
    rows, width = x_own.shape
    slots = hist_in.shape[0]
    piece = rows // 2
    q_tiles = w_all.shape[0] - 1
    tile = w_all.shape[2]
    half = tile // 2
    col_chunks, _, cols = w_out.shape
    side = col_chunks // 2
    nxt = lax.rem(section + 1, sections)
    prv = lax.rem(section + sections - 1, sections)

    load_x = start(pltpu.make_async_copy(x_hbm.at[0], x_own, x_sem))
    barrier = pltpu.get_barrier_semaphore()
    for other in (sibling, peer, (1 - hi) * 2 + (1 - lo)):
        pl.semaphore_signal(barrier, inc=1, device_id={"tensor": other}, device_id_type=MESH)
    for other in (nxt, prv):
        pl.semaphore_signal(barrier, inc=1, device_id={"section": other}, device_id_type=MESH)
    expected = jnp.int32(5)
    for k in range(1, slots + 1):
        step = DILATION_STRIDE * k
        forward, backward = section + step < sections, prv >= step

        @pl.when(forward)
        def _():
            pl.semaphore_signal(
                barrier,
                inc=1,
                device_id={"section": lax.rem(section + step + 1, sections)},
                device_id_type=MESH,
            )

        @pl.when(backward)
        def _():
            pl.semaphore_signal(
                barrier, inc=1, device_id={"section": prv - step}, device_id_type=MESH
            )

        expected = expected + forward.astype(jnp.int32) + backward.astype(jnp.int32)

    loads = []
    for j in range(q_tiles):
        loads.append(
            pltpu.make_async_copy(
                wq_hbm.at[0, :, pl.ds(j * tile, tile)], w_all.at[j], w_sem.at[j]
            )
        )
    loads.append(
        pltpu.make_async_copy(
            wk_hbm.at[0], w_all.at[q_tiles, :, pl.ds(0, half)], w_sem.at[q_tiles]
        )
    )
    loads.append(
        pltpu.make_async_copy(
            wv_hbm.at[0], w_all.at[q_tiles, :, pl.ds(half, half)], w_sem.at[q_tiles + 1]
        )
    )
    load_x.wait()
    for copy in loads:
        copy.start()
    load_mix = start(pltpu.make_async_copy(mix_hbm, mix_v, mix_sem))
    mine = pl.multiple_of(lo * rows, rows)

    def norm_rows(i, carry):
        at = pl.multiple_of(i * 16, 16)
        values = x_own[pl.ds(at, 16), :].astype(jnp.float32)
        inv = lax.rsqrt(jnp.mean(values * values, axis=-1, keepdims=True) + 1e-05)
        chip_rows[pl.ds(pl.multiple_of(mine + at, 16), 16), :] = (values * inv).astype(jnp.bfloat16)
        return carry

    lax.fori_loop(0, rows // 16, norm_rows, 0)
    pl.semaphore_wait(barrier, expected)

    def gather_copy(j):
        return pltpu.make_async_remote_copy(
            src_ref=chip_rows.at[pl.ds(pl.multiple_of(j * rows + lo * piece, piece), piece)],
            dst_ref=peer_rows.at[j, pl.ds(pl.multiple_of(lo * piece, piece), piece)],
            send_sem=gx_s.at[j],
            recv_sem=gx_r.at[j],
            device_id={"tensor": peer},
            device_id_type=MESH,
        )

    def forward_copy(j):
        place = peer_rows.at[j, pl.ds(pl.multiple_of(lo * piece, piece), piece)]
        return pltpu.make_async_remote_copy(
            src_ref=place,
            dst_ref=place,
            send_sem=fw_s.at[j],
            recv_sem=fw_r.at[j],
            device_id={"tensor": sibling},
            device_id_type=MESH,
        )

    def sibling_copy(i):
        which = 1 - lo if i == 0 else lo
        place = chip_rows.at[pl.ds(pl.multiple_of(mine + which * piece, piece), piece)]
        return pltpu.make_async_remote_copy(
            src_ref=place,
            dst_ref=place,
            send_sem=sib_s.at[i],
            recv_sem=sib_r.at[i],
            device_id={"tensor": sibling},
            device_id_type=MESH,
        )

    @pl.when(lo == 0)
    def _():
        gather_copy(0).start()

    for i in range(2):
        sibling_copy(i).start()
    sibling_copy(0).wait_recv()

    @pl.when(lo == 1)
    def _():
        gather_copy(0).start()

    gather_copy(1).start()

    def hist_copy(k):
        return pltpu.make_async_remote_copy(
            src_ref=hist_hbm.at[0, k - 1],
            dst_ref=hist_in.at[k - 1],
            send_sem=hist_s.at[k - 1],
            recv_sem=hist_r.at[k - 1],
            device_id={"section": lax.rem(section + DILATION_STRIDE * k + 1, sections)},
            device_id_type=MESH,
        )

    for k in range(1, slots + 1):
        step = DILATION_STRIDE * k

        @pl.when(section + step < sections)
        def _():
            hist_copy(k).start()

        @pl.when(prv < step)
        def _():
            hist_in[k - 1] = jnp.zeros((rows, width), hist_in.dtype)

    out_loads = []
    for c in range(col_chunks):
        out_loads.append(
            start(
                pltpu.make_async_copy(
                    wo_hbm.at[0, :, pl.ds(c * cols, cols)], w_out.at[c], wo_sem.at[c]
                )
            )
        )

    scale = 1.0 / math.sqrt(HEAD_DIM)

    def project(rows_ref, target):
        size = rows_ref.shape[0]
        where = pl.ds(pl.multiple_of(target, size), size)

        def q_tile(j, carry):
            acc = jnp.dot(rows_ref[...], w_all[j], preferred_element_type=jnp.float32)
            acc = acc.astype(jnp.bfloat16) * jnp.bfloat16(scale)
            q_all[2 * j, where, :] = acc[:, :half]
            q_all[2 * j + 1, where, :] = acc[:, half:]
            return carry

        lax.fori_loop(0, q_tiles, q_tile, 0)
        acc = jnp.dot(rows_ref[...], w_all[q_tiles], preferred_element_type=jnp.float32)
        acc = acc.astype(jnp.bfloat16).astype(jnp.float32)
        for part, padded in ((acc[:, :half], k_pad), (acc[:, half:], v_pad)):
            lane = lax.broadcasted_iota(jnp.int32, part.shape, 1)
            turned = pltpu.roll(part, HEAD_DIM, 1)
            low = lane < HEAD_DIM
            zero = jnp.zeros_like(part)
            forms = (
                jnp.where(low, part, zero),
                jnp.where(low, zero, turned),
                jnp.where(low, turned, zero),
                jnp.where(low, zero, part),
            )
            for f, form in enumerate(forms):
                padded[f, where, :] = form.astype(jnp.bfloat16)

    pairs = q_all.shape[0]
    pairs_per_kv = pairs // (half // HEAD_DIM)

    def attend(heads_ref, first, size, keys):
        def pair(p, carry):
            query = q_all[p, first : first + size, :]
            row_at = first + lax.broadcasted_iota(jnp.int32, (size, keys), 0)
            key_at = lax.broadcasted_iota(jnp.int32, (size, keys), 1)
            seen = row_at >= key_at
            kv = p // pairs_per_kv
            total = None
            for which in range(2):
                scores = lax.dot_general(
                    query,
                    k_pad[kv * 2 + which, :keys, :],
                    (((1,), (1,)), ((), ())),
                    preferred_element_type=jnp.float32,
                )
                scores = jnp.where(seen, scores, -1e30)
                top = jnp.max(scores, axis=-1, keepdims=True)
                weights = jnp.exp(scores - top)
                weights = weights * (1.0 / jnp.sum(weights, axis=-1, keepdims=True))
                term = jnp.dot(
                    weights.astype(jnp.bfloat16),
                    v_pad[kv * 2 + which, :keys, :],
                    preferred_element_type=jnp.float32,
                )
                total = term if total is None else total + term
            heads_ref[:, pl.ds(pl.multiple_of(p * half, half), half)] = total.astype(jnp.bfloat16)
            return carry

        lax.fori_loop(0, pairs, pair, 0)

    def give_copy(j, i):
        return pltpu.make_async_remote_copy(
            src_ref=peer_give.at[j, i],
            dst_ref=peer_got.at[j, i],
            send_sem=ps_s.at[j, i],
            recv_sem=ps_r.at[j, i],
            device_id={"tensor": sibling},
            device_id_type=MESH,
        )

    def cross_copy(j, i):
        return pltpu.make_async_remote_copy(
            src_ref=peer_keep.at[j, i],
            dst_ref=x_in.at[lo * side + i],
            send_sem=xs_s.at[j, i],
            recv_sem=xs_r.at[lo * side + i],
            device_id={"tensor": (1 - hi) * 2 + j},
            device_id_type=MESH,
        )

    def cross_arrival(c):
        return pltpu.make_async_remote_copy(
            src_ref=x_in.at[c],
            dst_ref=x_in.at[c],
            send_sem=xs_s.at[0, 0],
            recv_sem=xs_r.at[c],
            device_id={"tensor": peer},
            device_id_type=MESH,
        )

    def peer_output(j):
        def part(c):
            acc = jnp.dot(peer_heads[j], w_out[c], preferred_element_type=jnp.float32)
            return acc.astype(jnp.bfloat16)

        def step(i, carry):
            @pl.when(i < side)
            def _():
                peer_give[j, i] = part((1 - lo) * side + i)
                peer_keep[j, i] = part(lo * side + i)
                give_copy(j, i).start()

            @pl.when(i >= LAG)
            def _():
                at = i - LAG
                give_copy(j, at).wait_recv()
                total = peer_keep[j, at].astype(jnp.float32) + peer_got[j, at].astype(jnp.float32)
                peer_keep[j, at] = total.astype(jnp.bfloat16)
                cross_copy(j, at).start()

            return carry

        lax.fori_loop(0, side + LAG, step, 0)

    def own_copy(c):
        return pltpu.make_async_remote_copy(
            src_ref=own_parts.at[c, 1 - lo],
            dst_ref=own_got.at[c],
            send_sem=os_s.at[c],
            recv_sem=os_r.at[c],
            device_id={"tensor": sibling},
            device_id_type=MESH,
        )

    def own_part(c):
        acc = jnp.dot(own_heads[...], w_out[c], preferred_element_type=jnp.float32)
        acc = acc.astype(jnp.bfloat16)
        own_parts[c, 0] = acc[:rows]
        own_parts[c, 1] = acc[rows:]
        own_copy(c).start()

    def out_copy(c):
        return pltpu.make_async_remote_copy(
            src_ref=mixed.at[c],
            dst_ref=block_in.at[c],
            send_sem=out_s.at[c],
            recv_sem=out_r.at[c],
            device_id={"section": nxt},
            device_id_type=MESH,
        )

    for copy in loads:
        copy.wait()
    sibling_copy(1).wait_recv()
    project(chip_rows, hi * 2 * rows)
    for copy in out_loads:
        copy.wait()
    load_mix.wait()

    @pl.when(hi == 0)
    def _():
        attend(own_heads, 0, 2 * rows, 2 * rows)

        def own_step(c, carry):
            own_part(c)
            return carry

        lax.fori_loop(0, col_chunks, own_step, 0)

    for j in range(2):
        gather_copy(j).wait_recv()
        forward_copy(j).start()
        forward_copy(j).wait_recv()
        project(peer_rows.at[j], ((1 - hi) * 2 + j) * rows)

        @pl.when(hi == 0)
        def _():
            attend(peer_heads.at[j], (2 + j) * rows, rows, (3 + j) * rows)

        @pl.when(hi == 1)
        def _():
            attend(peer_heads.at[j], j * rows, rows, (1 + j) * rows)

        peer_output(j)

    @pl.when(hi == 1)
    def _():
        attend(own_heads, 2 * rows, 2 * rows, 4 * rows)

    def final_chunk(c):
        own_copy(c).wait_recv()
        total = own_parts[c, lo].astype(jnp.float32) + own_got[c].astype(jnp.float32)
        where = pl.ds(pl.multiple_of(c * cols, cols), cols)
        cross_arrival(c).wait_recv()
        total = total + x_in[c].astype(jnp.float32)
        block = (x_own[:, where].astype(jnp.float32) + total).astype(jnp.bfloat16)
        mixed[c] = block
        out_copy(c).start()

    def column(i):
        return (i % 2) * side + i // 2

    def final_step(i, carry):
        @pl.when((i < col_chunks) & (hi == 1))
        def _():
            own_part(column(i))

        @pl.when(i >= LAG)
        def _():
            final_chunk(column(i - LAG))

        return carry

    lax.fori_loop(0, col_chunks + LAG, final_step, 0)

    for k in range(1, slots + 1):

        @pl.when(prv >= DILATION_STRIDE * k)
        def _():
            hist_copy(k).wait_recv()

    def store_copy(c):
        return pltpu.make_async_copy(
            block_in.at[c],
            out_hbm.at[0, :, pl.ds(pl.multiple_of(c * cols, cols), cols)],
            store_sem.at[c],
        )

    def mix_step(i, carry):
        c = column(i)
        out_copy(c).wait_recv()
        where = pl.ds(pl.multiple_of(c * cols, cols), cols)
        factors = mix_v[pl.ds(prv, 1), :]
        value = factors[:, 0:1] * block_in[c].astype(jnp.float32)
        for k in range(1, slots + 1):
            past = hist_in[k - 1, :, where].astype(jnp.float32)
            value = value + factors[:, k : k + 1] * past
        block_in[c] = value.astype(jnp.bfloat16)
        store_copy(c).start()
        return carry

    lax.fori_loop(0, col_chunks, mix_step, 0)

    for i in range(2):
        sibling_copy(i).wait_send()
        gather_copy(i).wait_send()
        forward_copy(i).wait_send()
    for k in range(1, slots + 1):

        @pl.when(section + DILATION_STRIDE * k < sections)
        def _():
            hist_copy(k).wait_send()

    def drain(c, carry):
        j, i = c // side, c % side
        give_copy(j, i).wait_send()
        cross_copy(j, i).wait_send()
        own_copy(c).wait_send()
        out_copy(c).wait_send()
        store_copy(c).wait()
        return carry

    lax.fori_loop(0, col_chunks, drain, 0)


def solution(mesh):
    sections, tensor = mesh.shape["section"], mesh.shape["tensor"]
    assert tensor == 4
    col_chunks = 8

    def on_device(x, history, wq, wk, wv, wo, mix_weights):
        rows, width = x.shape[1:]
        slots = history.shape[1]
        q_width, kv_width = wq.shape[2], wk.shape[2]
        seq = rows * tensor
        tile = 2 * kv_width
        q_tiles = q_width // tile
        cols = width // col_chunks
        bf16 = jnp.bfloat16
        dma = pltpu.SemaphoreType.DMA
        hbm = pl.BlockSpec(memory_space=pl.ANY)
        return pl.pallas_call(
            functools.partial(tick_kernel, sections),
            out_shape=jax.ShapeDtypeStruct(x.shape, bf16),
            in_specs=[hbm] * 7,
            out_specs=hbm,
            scratch_shapes=[
                pltpu.VMEM((rows, width), bf16),
                pltpu.VMEM((2 * rows, width), bf16),
                pltpu.VMEM((2, rows, width), bf16),
                pltpu.VMEM((q_tiles + 1, width, tile), bf16),
                pltpu.VMEM((col_chunks, q_width, cols), bf16),
                pltpu.VMEM((2 * q_tiles, seq, kv_width), bf16),
                pltpu.VMEM((4, seq, kv_width), bf16),
                pltpu.VMEM((4, seq, kv_width), bf16),
                pltpu.VMEM((2, rows, q_width), bf16),
                pltpu.VMEM((2 * rows, q_width), bf16),
                pltpu.VMEM((2, col_chunks // 2, rows, cols), bf16),
                pltpu.VMEM((2, col_chunks // 2, rows, cols), bf16),
                pltpu.VMEM((2, col_chunks // 2, rows, cols), bf16),
                pltpu.VMEM((col_chunks, 2, rows, cols), bf16),
                pltpu.VMEM((col_chunks, rows, cols), bf16),
                pltpu.VMEM((col_chunks, rows, cols), bf16),
                pltpu.VMEM((col_chunks, rows, cols), bf16),
                pltpu.VMEM((slots, rows, width), bf16),
                pltpu.VMEM(mix_weights.shape, mix_weights.dtype),
                dma((q_tiles + 2,)),
                dma((col_chunks,)),
                dma,
                dma,
                dma((slots,)),
                dma((slots,)),
                dma((2,)),
                dma((2,)),
                dma((2,)),
                dma((2,)),
                dma((2,)),
                dma((2,)),
                dma((2, col_chunks // 2)),
                dma((2, col_chunks // 2)),
                dma((col_chunks,)),
                dma((col_chunks,)),
                dma((2, col_chunks // 2)),
                dma((col_chunks,)),
                dma((col_chunks,)),
                dma((col_chunks,)),
                pltpu.VMEM((col_chunks, rows, cols), bf16),
                dma((col_chunks,)),
            ],
            compiler_params=pltpu.CompilerParams(
                collective_id=0, has_side_effects=True, vmem_limit_bytes=60 * 1024 * 1024
            ),
        )(x, history, wq, wk, wv, wo, mix_weights)

    placed = (
        P("section", "tensor", None),
        P("section", None, "tensor", None),
        P("section", None, "tensor"),
        P("section", None, "tensor"),
        P("section", None, "tensor"),
        P("section", "tensor", None),
        P(),
    )
    return jax.shard_map(
        on_device,
        mesh=mesh,
        in_specs=placed,
        out_specs=P("section", "tensor", None),
        check_vma=False,
    )
```

```python
import functools
import math

import jax
import jax.numpy as jnp
from jax import lax
from jax.experimental import pallas as pl
from jax.experimental.pallas import tpu as pltpu
from jax.sharding import PartitionSpec as P

HEAD_DIM = 64
DILATION_STRIDE = 4
MESH = pl.DeviceIdType.MESH
LAG = 2


def start(copy):
    copy.start()
    return copy


def tick_kernel(
    sections,
    x_hbm,
    hist_hbm,
    wq_hbm,
    wk_hbm,
    wv_hbm,
    wo_hbm,
    mix_hbm,
    out_hbm,
    x_own,
    chip_rows,
    peer_rows,
    w_all,
    w_out,
    q_all,
    k_pad,
    v_pad,
    peer_heads,
    own_heads,
    peer_keep,
    peer_give,
    peer_got,
    own_parts,
    own_got,
    x_in,
    mixed,
    hist_in,
    mix_v,
    w_sem,
    wo_sem,
    x_sem,
    mix_sem,
    hist_s,
    hist_r,
    sib_s,
    sib_r,
    gx_s,
    gx_r,
    fw_s,
    fw_r,
    ps_s,
    ps_r,
    os_s,
    os_r,
    xs_s,
    xs_r,
    out_s,
    out_r,
    block_in,
    store_sem,
):
    section = lax.axis_index("section")
    me = lax.axis_index("tensor")
    hi, lo = me // 2, me % 2
    sibling = hi * 2 + (1 - lo)
    peer = (1 - hi) * 2 + lo
    rows, width = x_own.shape
    slots = hist_in.shape[0]
    piece = rows // 2
    q_tiles = w_all.shape[0] - 1
    tile = w_all.shape[2]
    half = tile // 2
    col_chunks, _, cols = w_out.shape
    side = col_chunks // 2
    nxt = lax.rem(section + 1, sections)
    prv = lax.rem(section + sections - 1, sections)

    load_x = start(pltpu.make_async_copy(x_hbm.at[0], x_own, x_sem))
    barrier = pltpu.get_barrier_semaphore()
    for other in (sibling, peer, (1 - hi) * 2 + (1 - lo)):
        pl.semaphore_signal(barrier, inc=1, device_id={"tensor": other}, device_id_type=MESH)
    for other in (nxt, prv):
        pl.semaphore_signal(barrier, inc=1, device_id={"section": other}, device_id_type=MESH)
    expected = jnp.int32(5)
    for k in range(1, slots + 1):
        step = DILATION_STRIDE * k
        forward, backward = section + step < sections, prv >= step

        @pl.when(forward)
        def _():
            pl.semaphore_signal(
                barrier,
                inc=1,
                device_id={"section": lax.rem(section + step + 1, sections)},
                device_id_type=MESH,
            )

        @pl.when(backward)
        def _():
            pl.semaphore_signal(
                barrier, inc=1, device_id={"section": prv - step}, device_id_type=MESH
            )

        expected = expected + forward.astype(jnp.int32) + backward.astype(jnp.int32)

    loads = []
    for j in range(q_tiles):
        loads.append(
            pltpu.make_async_copy(
                wq_hbm.at[0, :, pl.ds(j * tile, tile)], w_all.at[j], w_sem.at[j]
            )
        )
    loads.append(
        pltpu.make_async_copy(
            wk_hbm.at[0], w_all.at[q_tiles, :, pl.ds(0, half)], w_sem.at[q_tiles]
        )
    )
    loads.append(
        pltpu.make_async_copy(
            wv_hbm.at[0], w_all.at[q_tiles, :, pl.ds(half, half)], w_sem.at[q_tiles + 1]
        )
    )
    load_x.wait()
    for copy in loads:
        copy.start()
    load_mix = start(pltpu.make_async_copy(mix_hbm, mix_v, mix_sem))
    mine = pl.multiple_of(lo * rows, rows)

    def norm_rows(i, carry):
        at = pl.multiple_of(i * 16, 16)
        values = x_own[pl.ds(at, 16), :].astype(jnp.float32)
        inv = lax.rsqrt(jnp.mean(values * values, axis=-1, keepdims=True) + 1e-05)
        chip_rows[pl.ds(pl.multiple_of(mine + at, 16), 16), :] = (values * inv).astype(jnp.bfloat16)
        return carry

    lax.fori_loop(0, rows // 16, norm_rows, 0)
    pl.semaphore_wait(barrier, expected)

    def gather_copy(j):
        return pltpu.make_async_remote_copy(
            src_ref=chip_rows.at[pl.ds(pl.multiple_of(j * rows + lo * piece, piece), piece)],
            dst_ref=peer_rows.at[j, pl.ds(pl.multiple_of(lo * piece, piece), piece)],
            send_sem=gx_s.at[j],
            recv_sem=gx_r.at[j],
            device_id={"tensor": peer},
            device_id_type=MESH,
        )

    def forward_copy(j):
        place = peer_rows.at[j, pl.ds(pl.multiple_of(lo * piece, piece), piece)]
        return pltpu.make_async_remote_copy(
            src_ref=place,
            dst_ref=place,
            send_sem=fw_s.at[j],
            recv_sem=fw_r.at[j],
            device_id={"tensor": sibling},
            device_id_type=MESH,
        )

    def sibling_copy(i):
        which = 1 - lo if i == 0 else lo
        place = chip_rows.at[pl.ds(pl.multiple_of(mine + which * piece, piece), piece)]
        return pltpu.make_async_remote_copy(
            src_ref=place,
            dst_ref=place,
            send_sem=sib_s.at[i],
            recv_sem=sib_r.at[i],
            device_id={"tensor": sibling},
            device_id_type=MESH,
        )

    @pl.when(lo == 0)
    def _():
        gather_copy(0).start()

    for i in range(2):
        sibling_copy(i).start()
    sibling_copy(0).wait_recv()

    @pl.when(lo == 1)
    def _():
        gather_copy(0).start()

    gather_copy(1).start()

    def hist_copy(k):
        return pltpu.make_async_remote_copy(
            src_ref=hist_hbm.at[0, k - 1],
            dst_ref=hist_in.at[k - 1],
            send_sem=hist_s.at[k - 1],
            recv_sem=hist_r.at[k - 1],
            device_id={"section": lax.rem(section + DILATION_STRIDE * k + 1, sections)},
            device_id_type=MESH,
        )

    for k in range(1, slots + 1):
        step = DILATION_STRIDE * k

        @pl.when(section + step < sections)
        def _():
            hist_copy(k).start()

        @pl.when(prv < step)
        def _():
            hist_in[k - 1] = jnp.zeros((rows, width), hist_in.dtype)

    out_loads = []
    for c in range(col_chunks):
        out_loads.append(
            start(
                pltpu.make_async_copy(
                    wo_hbm.at[0, :, pl.ds(c * cols, cols)], w_out.at[c], wo_sem.at[c]
                )
            )
        )

    scale = 1.0 / math.sqrt(HEAD_DIM)

    def project_query(rows_ref, target):
        size = rows_ref.shape[0]
        where = pl.ds(pl.multiple_of(target, size), size)

        def q_tile(j, carry):
            acc = jnp.dot(rows_ref[...], w_all[j], preferred_element_type=jnp.float32)
            acc = acc.astype(jnp.bfloat16) * jnp.bfloat16(scale)
            q_all[2 * j, where, :] = acc[:, :half]
            q_all[2 * j + 1, where, :] = acc[:, half:]
            return carry

        lax.fori_loop(0, q_tiles, q_tile, 0)

    def project_key_value(rows_ref, target):
        size = rows_ref.shape[0]
        where = pl.ds(pl.multiple_of(target, size), size)
        acc = jnp.dot(rows_ref[...], w_all[q_tiles], preferred_element_type=jnp.float32)
        acc = acc.astype(jnp.bfloat16).astype(jnp.float32)
        for part, padded in ((acc[:, :half], k_pad), (acc[:, half:], v_pad)):
            lane = lax.broadcasted_iota(jnp.int32, part.shape, 1)
            turned = pltpu.roll(part, HEAD_DIM, 1)
            low = lane < HEAD_DIM
            zero = jnp.zeros_like(part)
            forms = (
                jnp.where(low, part, zero),
                jnp.where(low, zero, turned),
                jnp.where(low, turned, zero),
                jnp.where(low, zero, part),
            )
            for f, form in enumerate(forms):
                padded[f, where, :] = form.astype(jnp.bfloat16)

    pairs = q_all.shape[0]
    pairs_per_kv = pairs // (half // HEAD_DIM)

    def attend(heads_ref, first, size, keys):
        def pair(p, carry):
            query = q_all[p, first : first + size, :]
            row_at = first + lax.broadcasted_iota(jnp.int32, (size, keys), 0)
            key_at = lax.broadcasted_iota(jnp.int32, (size, keys), 1)
            seen = row_at >= key_at
            kv = p // pairs_per_kv
            total = None
            for which in range(2):
                scores = lax.dot_general(
                    query,
                    k_pad[kv * 2 + which, :keys, :],
                    (((1,), (1,)), ((), ())),
                    preferred_element_type=jnp.float32,
                )
                scores = jnp.where(seen, scores, -1e30)
                top = jnp.max(scores, axis=-1, keepdims=True)
                weights = jnp.exp(scores - top)
                weights = weights * (1.0 / jnp.sum(weights, axis=-1, keepdims=True))
                term = jnp.dot(
                    weights.astype(jnp.bfloat16),
                    v_pad[kv * 2 + which, :keys, :],
                    preferred_element_type=jnp.float32,
                )
                total = term if total is None else total + term
            heads_ref[:, pl.ds(pl.multiple_of(p * half, half), half)] = total.astype(jnp.bfloat16)
            return carry

        lax.fori_loop(0, pairs, pair, 0)

    def give_copy(j, i):
        return pltpu.make_async_remote_copy(
            src_ref=peer_give.at[j, i],
            dst_ref=peer_got.at[j, i],
            send_sem=ps_s.at[j, i],
            recv_sem=ps_r.at[j, i],
            device_id={"tensor": sibling},
            device_id_type=MESH,
        )

    def cross_copy(j, i):
        return pltpu.make_async_remote_copy(
            src_ref=peer_keep.at[j, i],
            dst_ref=x_in.at[lo * side + i],
            send_sem=xs_s.at[j, i],
            recv_sem=xs_r.at[lo * side + i],
            device_id={"tensor": (1 - hi) * 2 + j},
            device_id_type=MESH,
        )

    def cross_arrival(c):
        return pltpu.make_async_remote_copy(
            src_ref=x_in.at[c],
            dst_ref=x_in.at[c],
            send_sem=xs_s.at[0, 0],
            recv_sem=xs_r.at[c],
            device_id={"tensor": peer},
            device_id_type=MESH,
        )

    def peer_output(j):
        def part(c):
            acc = jnp.dot(peer_heads[j], w_out[c], preferred_element_type=jnp.float32)
            return acc.astype(jnp.bfloat16)

        def step(i, carry):
            @pl.when(i < side)
            def _():
                peer_give[j, i] = part((1 - lo) * side + i)
                peer_keep[j, i] = part(lo * side + i)
                give_copy(j, i).start()

            @pl.when(i >= LAG)
            def _():
                at = i - LAG
                give_copy(j, at).wait_recv()
                total = peer_keep[j, at].astype(jnp.float32) + peer_got[j, at].astype(jnp.float32)
                peer_keep[j, at] = total.astype(jnp.bfloat16)
                cross_copy(j, at).start()

            return carry

        lax.fori_loop(0, side + LAG, step, 0)

    def own_copy(c):
        return pltpu.make_async_remote_copy(
            src_ref=own_parts.at[c, 1 - lo],
            dst_ref=own_got.at[c],
            send_sem=os_s.at[c],
            recv_sem=os_r.at[c],
            device_id={"tensor": sibling},
            device_id_type=MESH,
        )

    def own_part(c):
        acc = jnp.dot(own_heads[...], w_out[c], preferred_element_type=jnp.float32)
        acc = acc.astype(jnp.bfloat16)
        own_parts[c, 0] = acc[:rows]
        own_parts[c, 1] = acc[rows:]
        own_copy(c).start()

    def out_copy(c):
        return pltpu.make_async_remote_copy(
            src_ref=mixed.at[c],
            dst_ref=block_in.at[c],
            send_sem=out_s.at[c],
            recv_sem=out_r.at[c],
            device_id={"section": nxt},
            device_id_type=MESH,
        )

    for copy in loads:
        copy.wait()
    sibling_copy(1).wait_recv()
    project_key_value(chip_rows, hi * 2 * rows)
    project_query(chip_rows, hi * 2 * rows)
    for copy in out_loads:
        copy.wait()
    load_mix.wait()

    @pl.when(hi == 0)
    def _():
        attend(own_heads, 0, 2 * rows, 2 * rows)

        def own_step(c, carry):
            own_part(c)
            return carry

        lax.fori_loop(0, col_chunks, own_step, 0)

    def final_chunk(c):
        own_copy(c).wait_recv()
        total = own_parts[c, lo].astype(jnp.float32) + own_got[c].astype(jnp.float32)
        where = pl.ds(pl.multiple_of(c * cols, cols), cols)
        cross_arrival(c).wait_recv()
        total = total + x_in[c].astype(jnp.float32)
        block = (x_own[:, where].astype(jnp.float32) + total).astype(jnp.bfloat16)
        mixed[c] = block
        out_copy(c).start()

    def column(i):
        return (i % 2) * side + i // 2

    def finish():
        def final_step(i, carry):
            final_chunk(column(i))
            return carry

        lax.fori_loop(0, col_chunks, final_step, 0)

    def peer_queries(j):
        project_query(peer_rows.at[j], ((1 - hi) * 2 + j) * rows)

        @pl.when(hi == 0)
        def _():
            attend(peer_heads.at[j], (2 + j) * rows, rows, (3 + j) * rows)

        @pl.when(hi == 1)
        def _():
            attend(peer_heads.at[j], j * rows, rows, (1 + j) * rows)

        peer_output(j)

    for j in range(2):
        gather_copy(j).wait_recv()
        forward_copy(j).start()
        forward_copy(j).wait_recv()
        project_key_value(peer_rows.at[j], ((1 - hi) * 2 + j) * rows)
        if j == 0:
            peer_queries(j)

    @pl.when(hi == 1)
    def _():
        attend(own_heads, 2 * rows, 2 * rows, 4 * rows)

        def own_step(i, carry):
            own_part(column(i))

            @pl.when((lo == 0) & (i >= LAG))
            def _():
                final_chunk(column(i - LAG))

            return carry

        lax.fori_loop(0, col_chunks, own_step, 0)

        @pl.when(lo == 0)
        def _():
            for i in range(col_chunks - LAG, col_chunks):
                final_chunk(column(i))

    peer_queries(1)

    @pl.when((hi == 0) | (lo == 1))
    def _():
        finish()

    for k in range(1, slots + 1):

        @pl.when(prv >= DILATION_STRIDE * k)
        def _():
            hist_copy(k).wait_recv()

    def store_copy(c):
        return pltpu.make_async_copy(
            block_in.at[c],
            out_hbm.at[0, :, pl.ds(pl.multiple_of(c * cols, cols), cols)],
            store_sem.at[c],
        )

    def mix_step(i, carry):
        c = column(i)
        out_copy(c).wait_recv()
        where = pl.ds(pl.multiple_of(c * cols, cols), cols)
        factors = mix_v[pl.ds(prv, 1), :]
        value = factors[:, 0:1] * block_in[c].astype(jnp.float32)
        for k in range(1, slots + 1):
            past = hist_in[k - 1, :, where].astype(jnp.float32)
            value = value + factors[:, k : k + 1] * past
        block_in[c] = value.astype(jnp.bfloat16)
        store_copy(c).start()
        return carry

    lax.fori_loop(0, col_chunks, mix_step, 0)

    for i in range(2):
        sibling_copy(i).wait_send()
        gather_copy(i).wait_send()
        forward_copy(i).wait_send()
    for k in range(1, slots + 1):

        @pl.when(section + DILATION_STRIDE * k < sections)
        def _():
            hist_copy(k).wait_send()

    def drain(c, carry):
        j, i = c // side, c % side
        give_copy(j, i).wait_send()
        cross_copy(j, i).wait_send()
        own_copy(c).wait_send()
        out_copy(c).wait_send()
        store_copy(c).wait()
        return carry

    lax.fori_loop(0, col_chunks, drain, 0)


def solution(mesh):
    sections, tensor = mesh.shape["section"], mesh.shape["tensor"]
    assert tensor == 4
    col_chunks = 8

    def on_device(x, history, wq, wk, wv, wo, mix_weights):
        rows, width = x.shape[1:]
        slots = history.shape[1]
        q_width, kv_width = wq.shape[2], wk.shape[2]
        seq = rows * tensor
        tile = 2 * kv_width
        q_tiles = q_width // tile
        cols = width // col_chunks
        bf16 = jnp.bfloat16
        dma = pltpu.SemaphoreType.DMA
        hbm = pl.BlockSpec(memory_space=pl.ANY)
        return pl.pallas_call(
            functools.partial(tick_kernel, sections),
            out_shape=jax.ShapeDtypeStruct(x.shape, bf16),
            in_specs=[hbm] * 7,
            out_specs=hbm,
            scratch_shapes=[
                pltpu.VMEM((rows, width), bf16),
                pltpu.VMEM((2 * rows, width), bf16),
                pltpu.VMEM((2, rows, width), bf16),
                pltpu.VMEM((q_tiles + 1, width, tile), bf16),
                pltpu.VMEM((col_chunks, q_width, cols), bf16),
                pltpu.VMEM((2 * q_tiles, seq, kv_width), bf16),
                pltpu.VMEM((4, seq, kv_width), bf16),
                pltpu.VMEM((4, seq, kv_width), bf16),
                pltpu.VMEM((2, rows, q_width), bf16),
                pltpu.VMEM((2 * rows, q_width), bf16),
                pltpu.VMEM((2, col_chunks // 2, rows, cols), bf16),
                pltpu.VMEM((2, col_chunks // 2, rows, cols), bf16),
                pltpu.VMEM((2, col_chunks // 2, rows, cols), bf16),
                pltpu.VMEM((col_chunks, 2, rows, cols), bf16),
                pltpu.VMEM((col_chunks, rows, cols), bf16),
                pltpu.VMEM((col_chunks, rows, cols), bf16),
                pltpu.VMEM((col_chunks, rows, cols), bf16),
                pltpu.VMEM((slots, rows, width), bf16),
                pltpu.VMEM(mix_weights.shape, mix_weights.dtype),
                dma((q_tiles + 2,)),
                dma((col_chunks,)),
                dma,
                dma,
                dma((slots,)),
                dma((slots,)),
                dma((2,)),
                dma((2,)),
                dma((2,)),
                dma((2,)),
                dma((2,)),
                dma((2,)),
                dma((2, col_chunks // 2)),
                dma((2, col_chunks // 2)),
                dma((col_chunks,)),
                dma((col_chunks,)),
                dma((2, col_chunks // 2)),
                dma((col_chunks,)),
                dma((col_chunks,)),
                dma((col_chunks,)),
                pltpu.VMEM((col_chunks, rows, cols), bf16),
                dma((col_chunks,)),
            ],
            compiler_params=pltpu.CompilerParams(
                collective_id=0, has_side_effects=True, vmem_limit_bytes=60 * 1024 * 1024
            ),
        )(x, history, wq, wk, wv, wo, mix_weights)

    placed = (
        P("section", "tensor", None),
        P("section", None, "tensor", None),
        P("section", None, "tensor"),
        P("section", None, "tensor"),
        P("section", None, "tensor"),
        P("section", "tensor", None),
        P(),
    )
    return jax.shard_map(
        on_device,
        mesh=mesh,
        in_specs=placed,
        out_specs=P("section", "tensor", None),
        check_vma=False,
    )
```

```python
import functools
import math

import jax
import jax.numpy as jnp
from jax import lax
from jax.experimental import pallas as pl
from jax.experimental.pallas import tpu as pltpu
from jax.sharding import PartitionSpec as P

HEAD_DIM = 64
DILATION_STRIDE = 4
MESH = pl.DeviceIdType.MESH
LAG = 2


def start(copy):
    copy.start()
    return copy


def tick_kernel(
    sections,
    x_hbm,
    hist_hbm,
    wq_hbm,
    wk_hbm,
    wv_hbm,
    wo_hbm,
    mix_hbm,
    out_hbm,
    x_own,
    chip_rows,
    peer_rows,
    w_all,
    w_out,
    q_all,
    k_pad,
    v_pad,
    peer_heads,
    own_heads,
    peer_keep,
    peer_give,
    peer_got,
    own_parts,
    own_got,
    x_in,
    mixed,
    hist_in,
    mix_v,
    w_sem,
    wo_sem,
    x_sem,
    mix_sem,
    hist_s,
    hist_r,
    sib_s,
    sib_r,
    gx_s,
    gx_r,
    fw_s,
    fw_r,
    ps_s,
    ps_r,
    os_s,
    os_r,
    xs_s,
    xs_r,
    out_s,
    out_r,
    block_in,
    store_sem,
):
    section = lax.axis_index("section")
    me = lax.axis_index("tensor")
    hi, lo = me // 2, me % 2
    sibling = hi * 2 + (1 - lo)
    peer = (1 - hi) * 2 + lo
    rows, width = x_own.shape
    slots = hist_in.shape[0]
    piece = rows // 2
    q_tiles = w_all.shape[0] - 1
    tile = w_all.shape[2]
    half = tile // 2
    col_chunks, _, cols = w_out.shape
    side = col_chunks // 2
    nxt = lax.rem(section + 1, sections)
    prv = lax.rem(section + sections - 1, sections)

    load_x = start(pltpu.make_async_copy(x_hbm.at[0], x_own, x_sem))
    barrier = pltpu.get_barrier_semaphore()
    for other in (sibling, peer, (1 - hi) * 2 + (1 - lo)):
        pl.semaphore_signal(barrier, inc=1, device_id={"tensor": other}, device_id_type=MESH)
    for other in (nxt, prv):
        pl.semaphore_signal(barrier, inc=1, device_id={"section": other}, device_id_type=MESH)
    expected = jnp.int32(5)
    for k in range(1, slots + 1):
        step = DILATION_STRIDE * k
        forward, backward = section + step < sections, prv >= step

        @pl.when(forward)
        def _():
            pl.semaphore_signal(
                barrier,
                inc=1,
                device_id={"section": lax.rem(section + step + 1, sections)},
                device_id_type=MESH,
            )

        @pl.when(backward)
        def _():
            pl.semaphore_signal(
                barrier, inc=1, device_id={"section": prv - step}, device_id_type=MESH
            )

        expected = expected + forward.astype(jnp.int32) + backward.astype(jnp.int32)

    loads = []
    for j in range(q_tiles):
        loads.append(
            pltpu.make_async_copy(
                wq_hbm.at[0, :, pl.ds(j * tile, tile)], w_all.at[j], w_sem.at[j]
            )
        )
    loads.append(
        pltpu.make_async_copy(
            wk_hbm.at[0], w_all.at[q_tiles, :, pl.ds(0, half)], w_sem.at[q_tiles]
        )
    )
    loads.append(
        pltpu.make_async_copy(
            wv_hbm.at[0], w_all.at[q_tiles, :, pl.ds(half, half)], w_sem.at[q_tiles + 1]
        )
    )
    load_x.wait()
    for copy in loads:
        copy.start()
    load_mix = start(pltpu.make_async_copy(mix_hbm, mix_v, mix_sem))
    mine = pl.multiple_of(lo * rows, rows)

    def norm_rows(i, carry):
        at = pl.multiple_of(i * 16, 16)
        values = x_own[pl.ds(at, 16), :].astype(jnp.float32)
        inv = lax.rsqrt(jnp.mean(values * values, axis=-1, keepdims=True) + 1e-05)
        chip_rows[pl.ds(pl.multiple_of(mine + at, 16), 16), :] = (values * inv).astype(jnp.bfloat16)
        return carry

    lax.fori_loop(0, rows // 16, norm_rows, 0)
    pl.semaphore_wait(barrier, expected)

    def gather_copy(j):
        return pltpu.make_async_remote_copy(
            src_ref=chip_rows.at[pl.ds(pl.multiple_of(j * rows + lo * piece, piece), piece)],
            dst_ref=peer_rows.at[j, pl.ds(pl.multiple_of(lo * piece, piece), piece)],
            send_sem=gx_s.at[j],
            recv_sem=gx_r.at[j],
            device_id={"tensor": peer},
            device_id_type=MESH,
        )

    def forward_copy(j):
        place = peer_rows.at[j, pl.ds(pl.multiple_of(lo * piece, piece), piece)]
        return pltpu.make_async_remote_copy(
            src_ref=place,
            dst_ref=place,
            send_sem=fw_s.at[j],
            recv_sem=fw_r.at[j],
            device_id={"tensor": sibling},
            device_id_type=MESH,
        )

    def sibling_copy(i):
        which = 1 - lo if i == 0 else lo
        place = chip_rows.at[pl.ds(pl.multiple_of(mine + which * piece, piece), piece)]
        return pltpu.make_async_remote_copy(
            src_ref=place,
            dst_ref=place,
            send_sem=sib_s.at[i],
            recv_sem=sib_r.at[i],
            device_id={"tensor": sibling},
            device_id_type=MESH,
        )

    @pl.when(lo == 0)
    def _():
        gather_copy(0).start()

    for i in range(2):
        sibling_copy(i).start()
    sibling_copy(0).wait_recv()

    @pl.when(lo == 1)
    def _():
        gather_copy(0).start()

    gather_copy(1).start()

    def hist_copy(k):
        return pltpu.make_async_remote_copy(
            src_ref=hist_hbm.at[0, k - 1],
            dst_ref=hist_in.at[k - 1],
            send_sem=hist_s.at[k - 1],
            recv_sem=hist_r.at[k - 1],
            device_id={"section": lax.rem(section + DILATION_STRIDE * k + 1, sections)},
            device_id_type=MESH,
        )

    for k in range(1, slots + 1):
        step = DILATION_STRIDE * k

        @pl.when(section + step < sections)
        def _():
            hist_copy(k).start()

        @pl.when(prv < step)
        def _():
            hist_in[k - 1] = jnp.zeros((rows, width), hist_in.dtype)

    out_loads = []
    for c in range(col_chunks):
        out_loads.append(
            start(
                pltpu.make_async_copy(
                    wo_hbm.at[0, :, pl.ds(c * cols, cols)], w_out.at[c], wo_sem.at[c]
                )
            )
        )

    scale = 1.0 / math.sqrt(HEAD_DIM)

    def project_query(rows_ref, target):
        size = rows_ref.shape[0]
        where = pl.ds(pl.multiple_of(target, size), size)

        def q_tile(j, carry):
            acc = jnp.dot(rows_ref[...], w_all[j], preferred_element_type=jnp.float32)
            acc = acc.astype(jnp.bfloat16) * jnp.bfloat16(scale)
            q_all[2 * j, where, :] = acc[:, :half]
            q_all[2 * j + 1, where, :] = acc[:, half:]
            return carry

        lax.fori_loop(0, q_tiles, q_tile, 0)

    def project_key_value(rows_ref, target):
        size = rows_ref.shape[0]
        where = pl.ds(pl.multiple_of(target, size), size)
        acc = jnp.dot(rows_ref[...], w_all[q_tiles], preferred_element_type=jnp.float32)
        acc = acc.astype(jnp.bfloat16).astype(jnp.float32)
        for part, padded in ((acc[:, :half], k_pad), (acc[:, half:], v_pad)):
            lane = lax.broadcasted_iota(jnp.int32, part.shape, 1)
            turned = pltpu.roll(part, HEAD_DIM, 1)
            low = lane < HEAD_DIM
            zero = jnp.zeros_like(part)
            forms = (
                jnp.where(low, part, zero),
                jnp.where(low, zero, turned),
                jnp.where(low, turned, zero),
                jnp.where(low, zero, part),
            )
            for f, form in enumerate(forms):
                padded[f, where, :] = form.astype(jnp.bfloat16)

    pairs = q_all.shape[0]
    pairs_per_kv = pairs // (half // HEAD_DIM)

    def attend(heads_ref, first, size, keys):
        def pair(p, carry):
            query = q_all[p, first : first + size, :]
            row_at = first + lax.broadcasted_iota(jnp.int32, (size, keys), 0)
            key_at = lax.broadcasted_iota(jnp.int32, (size, keys), 1)
            seen = row_at >= key_at
            kv = p // pairs_per_kv
            total = None
            for which in range(2):
                scores = lax.dot_general(
                    query,
                    k_pad[kv * 2 + which, :keys, :],
                    (((1,), (1,)), ((), ())),
                    preferred_element_type=jnp.float32,
                )
                scores = jnp.where(seen, scores, -1e30)
                top = jnp.max(scores, axis=-1, keepdims=True)
                weights = jnp.exp(scores - top)
                weights = weights * (1.0 / jnp.sum(weights, axis=-1, keepdims=True))
                term = jnp.dot(
                    weights.astype(jnp.bfloat16),
                    v_pad[kv * 2 + which, :keys, :],
                    preferred_element_type=jnp.float32,
                )
                total = term if total is None else total + term
            heads_ref[:, pl.ds(pl.multiple_of(p * half, half), half)] = total.astype(jnp.bfloat16)
            return carry

        lax.fori_loop(0, pairs, pair, 0)

    def give_copy(j, i):
        return pltpu.make_async_remote_copy(
            src_ref=peer_give.at[j, i],
            dst_ref=peer_got.at[j, i],
            send_sem=ps_s.at[j, i],
            recv_sem=ps_r.at[j, i],
            device_id={"tensor": sibling},
            device_id_type=MESH,
        )

    def cross_copy(j, i):
        return pltpu.make_async_remote_copy(
            src_ref=peer_keep.at[j, i],
            dst_ref=x_in.at[lo * side + i],
            send_sem=xs_s.at[j, i],
            recv_sem=xs_r.at[lo * side + i],
            device_id={"tensor": (1 - hi) * 2 + j},
            device_id_type=MESH,
        )

    def cross_arrival(c):
        return pltpu.make_async_remote_copy(
            src_ref=x_in.at[c],
            dst_ref=x_in.at[c],
            send_sem=xs_s.at[0, 0],
            recv_sem=xs_r.at[c],
            device_id={"tensor": peer},
            device_id_type=MESH,
        )

    def peer_output(j):
        def part(c):
            acc = jnp.dot(peer_heads[j], w_out[c], preferred_element_type=jnp.float32)
            return acc.astype(jnp.bfloat16)

        def step(i, carry):
            @pl.when(i < side)
            def _():
                peer_give[j, i] = part((1 - lo) * side + i)
                peer_keep[j, i] = part(lo * side + i)
                give_copy(j, i).start()

            @pl.when(i >= LAG)
            def _():
                at = i - LAG
                give_copy(j, at).wait_recv()
                total = peer_keep[j, at].astype(jnp.float32) + peer_got[j, at].astype(jnp.float32)
                peer_keep[j, at] = total.astype(jnp.bfloat16)
                cross_copy(j, at).start()

            return carry

        lax.fori_loop(0, side + LAG, step, 0)

    def own_copy(c):
        return pltpu.make_async_remote_copy(
            src_ref=own_parts.at[c, 1 - lo],
            dst_ref=own_got.at[c],
            send_sem=os_s.at[c],
            recv_sem=os_r.at[c],
            device_id={"tensor": sibling},
            device_id_type=MESH,
        )

    def own_part(c):
        acc = jnp.dot(own_heads[...], w_out[c], preferred_element_type=jnp.float32)
        acc = acc.astype(jnp.bfloat16)
        own_parts[c, 0] = acc[:rows]
        own_parts[c, 1] = acc[rows:]
        own_copy(c).start()

    def out_copy(c):
        return pltpu.make_async_remote_copy(
            src_ref=mixed.at[c],
            dst_ref=block_in.at[c],
            send_sem=out_s.at[c],
            recv_sem=out_r.at[c],
            device_id={"section": nxt},
            device_id_type=MESH,
        )

    for copy in loads:
        copy.wait()
    sibling_copy(1).wait_recv()
    project_key_value(chip_rows, hi * 2 * rows)
    project_query(chip_rows, hi * 2 * rows)
    for copy in out_loads:
        copy.wait()
    load_mix.wait()

    @pl.when(hi == 0)
    def _():
        attend(own_heads, 0, 2 * rows, 2 * rows)

        def own_step(c, carry):
            own_part(c)
            return carry

        lax.fori_loop(0, col_chunks, own_step, 0)

    def final_chunk(c):
        own_copy(c).wait_recv()
        total = own_parts[c, lo].astype(jnp.float32) + own_got[c].astype(jnp.float32)
        where = pl.ds(pl.multiple_of(c * cols, cols), cols)
        cross_arrival(c).wait_recv()
        total = total + x_in[c].astype(jnp.float32)
        block = (x_own[:, where].astype(jnp.float32) + total).astype(jnp.bfloat16)
        mixed[c] = block
        out_copy(c).start()

    def column(i):
        return (i % 2) * side + i // 2

    def finish():
        def final_step(i, carry):
            final_chunk(column(i))
            return carry

        lax.fori_loop(0, col_chunks, final_step, 0)

    def peer_queries(j):
        project_query(peer_rows.at[j], ((1 - hi) * 2 + j) * rows)

        @pl.when(hi == 0)
        def _():
            attend(peer_heads.at[j], (2 + j) * rows, rows, (3 + j) * rows)

        @pl.when(hi == 1)
        def _():
            attend(peer_heads.at[j], j * rows, rows, (1 + j) * rows)

        if j == 1:

            @pl.when((hi == 0) & (lo == 0))
            def _():
                finish()

        peer_output(j)

    for j in range(2):
        gather_copy(j).wait_recv()
        forward_copy(j).start()
        forward_copy(j).wait_recv()
        project_key_value(peer_rows.at[j], ((1 - hi) * 2 + j) * rows)
        if j == 0:
            peer_queries(j)

    @pl.when(hi == 1)
    def _():
        attend(own_heads, 2 * rows, 2 * rows, 4 * rows)

        def own_step(i, carry):
            own_part(column(i))

            @pl.when((lo == 0) & (i >= LAG))
            def _():
                final_chunk(column(i - LAG))

            return carry

        lax.fori_loop(0, col_chunks, own_step, 0)

        @pl.when(lo == 0)
        def _():
            for i in range(col_chunks - LAG, col_chunks):
                final_chunk(column(i))

    peer_queries(1)

    @pl.when(lo == 1)
    def _():
        finish()

    for k in range(1, slots + 1):

        @pl.when(prv >= DILATION_STRIDE * k)
        def _():
            hist_copy(k).wait_recv()

    def store_copy(c):
        return pltpu.make_async_copy(
            block_in.at[c],
            out_hbm.at[0, :, pl.ds(pl.multiple_of(c * cols, cols), cols)],
            store_sem.at[c],
        )

    def mix_step(i, carry):
        c = column(i)
        out_copy(c).wait_recv()
        where = pl.ds(pl.multiple_of(c * cols, cols), cols)
        factors = mix_v[pl.ds(prv, 1), :]
        value = factors[:, 0:1] * block_in[c].astype(jnp.float32)
        for k in range(1, slots + 1):
            past = hist_in[k - 1, :, where].astype(jnp.float32)
            value = value + factors[:, k : k + 1] * past
        block_in[c] = value.astype(jnp.bfloat16)
        store_copy(c).start()
        return carry

    lax.fori_loop(0, col_chunks, mix_step, 0)

    for i in range(2):
        sibling_copy(i).wait_send()
        gather_copy(i).wait_send()
        forward_copy(i).wait_send()
    for k in range(1, slots + 1):

        @pl.when(section + DILATION_STRIDE * k < sections)
        def _():
            hist_copy(k).wait_send()

    def drain(c, carry):
        j, i = c // side, c % side
        give_copy(j, i).wait_send()
        cross_copy(j, i).wait_send()
        own_copy(c).wait_send()
        out_copy(c).wait_send()
        store_copy(c).wait()
        return carry

    lax.fori_loop(0, col_chunks, drain, 0)


def solution(mesh):
    sections, tensor = mesh.shape["section"], mesh.shape["tensor"]
    assert tensor == 4
    col_chunks = 8

    def on_device(x, history, wq, wk, wv, wo, mix_weights):
        rows, width = x.shape[1:]
        slots = history.shape[1]
        q_width, kv_width = wq.shape[2], wk.shape[2]
        seq = rows * tensor
        tile = 2 * kv_width
        q_tiles = q_width // tile
        cols = width // col_chunks
        bf16 = jnp.bfloat16
        dma = pltpu.SemaphoreType.DMA
        hbm = pl.BlockSpec(memory_space=pl.ANY)
        return pl.pallas_call(
            functools.partial(tick_kernel, sections),
            out_shape=jax.ShapeDtypeStruct(x.shape, bf16),
            in_specs=[hbm] * 7,
            out_specs=hbm,
            scratch_shapes=[
                pltpu.VMEM((rows, width), bf16),
                pltpu.VMEM((2 * rows, width), bf16),
                pltpu.VMEM((2, rows, width), bf16),
                pltpu.VMEM((q_tiles + 1, width, tile), bf16),
                pltpu.VMEM((col_chunks, q_width, cols), bf16),
                pltpu.VMEM((2 * q_tiles, seq, kv_width), bf16),
                pltpu.VMEM((4, seq, kv_width), bf16),
                pltpu.VMEM((4, seq, kv_width), bf16),
                pltpu.VMEM((2, rows, q_width), bf16),
                pltpu.VMEM((2 * rows, q_width), bf16),
                pltpu.VMEM((2, col_chunks // 2, rows, cols), bf16),
                pltpu.VMEM((2, col_chunks // 2, rows, cols), bf16),
                pltpu.VMEM((2, col_chunks // 2, rows, cols), bf16),
                pltpu.VMEM((col_chunks, 2, rows, cols), bf16),
                pltpu.VMEM((col_chunks, rows, cols), bf16),
                pltpu.VMEM((col_chunks, rows, cols), bf16),
                pltpu.VMEM((col_chunks, rows, cols), bf16),
                pltpu.VMEM((slots, rows, width), bf16),
                pltpu.VMEM(mix_weights.shape, mix_weights.dtype),
                dma((q_tiles + 2,)),
                dma((col_chunks,)),
                dma,
                dma,
                dma((slots,)),
                dma((slots,)),
                dma((2,)),
                dma((2,)),
                dma((2,)),
                dma((2,)),
                dma((2,)),
                dma((2,)),
                dma((2, col_chunks // 2)),
                dma((2, col_chunks // 2)),
                dma((col_chunks,)),
                dma((col_chunks,)),
                dma((2, col_chunks // 2)),
                dma((col_chunks,)),
                dma((col_chunks,)),
                dma((col_chunks,)),
                pltpu.VMEM((col_chunks, rows, cols), bf16),
                dma((col_chunks,)),
            ],
            compiler_params=pltpu.CompilerParams(
                collective_id=0, has_side_effects=True, vmem_limit_bytes=60 * 1024 * 1024
            ),
        )(x, history, wq, wk, wv, wo, mix_weights)

    placed = (
        P("section", "tensor", None),
        P("section", None, "tensor", None),
        P("section", None, "tensor"),
        P("section", None, "tensor"),
        P("section", None, "tensor"),
        P("section", "tensor", None),
        P(),
    )
    return jax.shard_map(
        on_device,
        mesh=mesh,
        in_specs=placed,
        out_specs=P("section", "tensor", None),
        check_vma=False,
    )
```
